32 devices in a mesh: blk: 8 (over z, y), grp: 4 (over x, core).
Axes of the slice: x: 2, y: 2, z: 4, core: 2. Of those that a mesh axis runs over, the one named last changes fastest.
Arguments:
- image_emb: bfloat16 [12288, 1152], P(('blk', 'grp')), may hold values from -0.1875 to 0.1875
- text_emb: bfloat16 [12288, 1152], P(('blk', 'grp')), may hold values from -0.1875 to 0.1875
- positives: int32 [32, 384], P(('blk', 'grp')), may hold values from 0 to 383, each once within a row
- pair_mask: int32 [8, 7], replicated, may hold values from 0 to 1, as said below
- log_scale: float32 [1], replicated, may hold values from 1.5 to 2.5
- bias: float32 [1], replicated, may hold values from -3 to -1
Outputs:
- image_grad: bfloat16 [12288, 1152], P(('blk', 'grp'))
- text_grad: bfloat16 [12288, 1152], P(('blk', 'grp'))
- loss: float32 [1], replicated
The draws below stay inside these ranges and needn't reach their ends.
Inputs may be any that keep to these rules, and one draw needn't show every extreme that they name: `positives`: every row is a permutation of the rows of a block. `pair_mask`: column 3 is 1 in every row (each image block is scored against its own text block); at least one row is all ones.
All inputs are finite; a program needn't handle non-finite values.
Results may differ from the reference program's by a relative error of at most 0.0063.
Values may be sent and summed in bfloat16 or wider, within the bound.
A program may use at most 64 MiB of HBM per device.

```python
import jax
import jax.numpy as jnp
from jax import lax

D = 1152
ROWS = 384
REACH = 3
IMAGES = 12288
N_BLK = 8
N_GRP = 4


def draw_pair_mask(key, part):
    first_key = jax.random.fold_in(key, 11)
    second_key = jax.random.fold_in(key, 23)
    coins = jax.random.randint(first_key, (N_BLK, 2 * REACH + 1), 0, 4)
    chosen = jnp.where(coins == 0, 1, 0).astype(jnp.int32)
    full_row = jax.random.randint(second_key, (), 0, N_BLK)
    row_index = lax.broadcasted_iota(jnp.int32, (N_BLK, 2 * REACH + 1), 0)
    col_index = lax.broadcasted_iota(jnp.int32, (N_BLK, 2 * REACH + 1), 1)
    chosen = jnp.where(row_index == full_row, 1, chosen)
    chosen = jnp.where(col_index == REACH, 1, chosen)
    return chosen.astype(jnp.int32)


def shard_levels(key, shape, pieces, least, high):
    level, own = 1.0, jax.random.fold_in(key, 6)
    for position, blocks in pieces:
        steps = jnp.exp(jax.random.uniform(jax.random.fold_in(own, position), (blocks,), jnp.float32, least / len(pieces), high / len(pieces)))
        level = level * jnp.repeat(steps, shape[position] // blocks).reshape([-1 if axis == position else 1 for axis in range(len(shape))])
    return level


def centred(own_key, dims, width, limit, shards=(), dtype=jnp.bfloat16):
    array = jax.random.normal(own_key, dims, jnp.float32) * width
    if len(shards) > 0:
        array = shard_levels(own_key, dims, shards, -0.22, 0.18) * array
    return jnp.clip(array, min=-limit, max=limit).astype(dtype)


def setup_inputs(seed: int = 0) -> dict:
    splits = jax.random.split(jax.random.key(seed), 7)
    image_emb = centred(splits[0], (IMAGES, D), D ** -0.5, 0.1875, ((0, 32),))
    text_emb = centred(splits[1], (IMAGES, D), D ** -0.5, 0.1875, ((0, 32),))
    positives = jax.vmap(lambda own: jax.random.permutation(own, ROWS))(jax.random.split(splits[2], (N_BLK * N_GRP))).reshape((N_BLK * N_GRP, ROWS)).astype(jnp.int32)
    pair_mask = draw_pair_mask(jax.random.fold_in(splits[6], 71), 0)
    log_scale = jnp.clip(jax.random.uniform(splits[4], (1,), jnp.float32, 1.5, 2.5), 1.5, 2.5)
    bias = jnp.clip(jax.random.uniform(splits[5], (1,), jnp.float32, -3.0, -1.0), -3.0, -1.0)
    return {"image_emb": image_emb, "text_emb": text_emb, "positives": positives, "pair_mask": pair_mask, "log_scale": log_scale, "bias": bias}


epsilon = 1e-06

def unit_rows(embedded):
    values = embedded.astype(jnp.float32)
    length = jnp.sqrt(lax.optimization_barrier(jnp.sum(values * values, axis=1, keepdims=True)) + epsilon)
    return (values / length, length)

def back_rows(normed, length, upstream):
    inward = lax.optimization_barrier(jnp.sum(normed * upstream, axis=1, keepdims=True))
    return (upstream - normed * inward) / length

def score_tile(image_side, text_side, labels, logit_scale, offset):
    similar = jnp.einsum('rd,cd->rc', image_side, text_side, preferred_element_type=jnp.float32)
    logits = logit_scale * similar + offset
    signed = labels * logits
    loss_sum = jnp.sum(jax.nn.softplus(-signed))
    slopes = (-labels * jax.nn.sigmoid(-signed) * logit_scale).astype(jnp.bfloat16)
    return (slopes, loss_sum)

def masked_tile(active_flag, image_side, text_side, labels, logit_scale, offset):

    def active(unused):
        return score_tile(image_side, text_side, labels, logit_scale, offset)

    def skipped(unused):
        return (jnp.zeros((image_side.shape[0], text_side.shape[0]), jnp.bfloat16), jnp.zeros((), jnp.float32))
    return lax.cond(active_flag > 0, active, skipped, 0)

def reference(image_emb, text_emb, positives, pair_mask, log_scale, bias):
    logit_scale = jnp.exp(log_scale[0])
    offset = bias[0]
    image_normed, image_len = unit_rows(image_emb)
    text_normed, text_len = unit_rows(text_emb)
    block_count = N_BLK * N_GRP
    image_blocks = image_normed.astype(jnp.bfloat16).reshape(block_count, ROWS, D)
    text_blocks = text_normed.astype(jnp.bfloat16).reshape(N_BLK, N_GRP, ROWS, D)
    columns = lax.broadcasted_iota(jnp.int32, (ROWS, ROWS), 1)
    image_total = jnp.zeros((block_count, ROWS, D), jnp.float32)
    text_total = jnp.zeros((N_BLK, N_GRP, ROWS, D), jnp.float32)
    loss_total = jnp.zeros((), jnp.float32)
    for distance in range(-REACH, REACH + 1):
        partner = jnp.roll(text_blocks, -distance, axis=0).reshape(block_count, ROWS, D)
        flags = jnp.broadcast_to(pair_mask[:, REACH + distance][:, None], (N_BLK, N_GRP)).reshape(block_count)

        def one_block(items, distance=distance):
            image_side, text_side, active_flag, matches = items
            if distance == 0:
                labels = jnp.where(matches[:, None] == columns, 1.0, -1.0).astype(jnp.float32)
            else:
                labels = -jnp.ones((ROWS, ROWS), jnp.float32)
            slopes, part_loss = masked_tile(active_flag, image_side, text_side, labels, logit_scale, offset)
            image_part = jnp.dot(slopes, text_side, preferred_element_type=jnp.float32)
            text_part = jnp.einsum('rc,rd->cd', slopes, image_side, preferred_element_type=jnp.float32)
            if distance != 0:
                text_part = lax.optimization_barrier(text_part.astype(jnp.bfloat16)).astype(jnp.float32)
            return (image_part, text_part, part_loss)
        image_part, text_part, parts = lax.map(one_block, (image_blocks, partner, flags, positives))
        image_total = image_total + image_part
        text_total = text_total + jnp.roll(text_part.reshape(N_BLK, N_GRP, ROWS, D), distance, axis=0)
        loss_total = loss_total + jnp.sum(parts)
    image_grad = back_rows(image_normed, image_len, image_total.reshape(IMAGES, D)).astype(jnp.bfloat16)
    text_grad = back_rows(text_normed, text_len, text_total.reshape(IMAGES, D)).astype(jnp.bfloat16)
    loss = (loss_total / IMAGES).reshape(1)
    return (image_grad, text_grad, loss)
```

```python
import functools

import jax
import jax.numpy as jnp
from jax import lax
from jax.experimental import pallas as pl
from jax.experimental.pallas import tpu as pltpu
from jax.sharding import PartitionSpec as P

epsilon = 1e-06


def passed_along(value, axis, steps):
    count = lax.axis_size(axis)
    pairs = [(source, (source + steps) % count) for source in range(count)]
    return lax.ppermute(value, axis, pairs)


def unit_rows(embedded):
    values = embedded.astype(jnp.float32)
    length = jnp.sqrt(jnp.sum(values * values, axis=1, keepdims=True) + epsilon)
    return (values / length, length)


def back_rows(normed, length, upstream):
    inward = jnp.sum(normed * upstream, axis=1, keepdims=True)
    return (upstream - normed * inward) / length


def score_tile(image_side, text_side, labels, logit_scale, offset):
    similar = jnp.einsum("rd,cd->rc", image_side, text_side, preferred_element_type=jnp.float32)
    logits = logit_scale * similar + offset
    signed = labels * logits
    loss_sum = jnp.sum(jax.nn.softplus(-signed))
    slopes = (-labels * jax.nn.sigmoid(-signed) * logit_scale).astype(jnp.bfloat16)
    return (slopes, loss_sum)


def masked_tile(active_flag, image_side, text_side, labels, logit_scale, offset):

    def active(unused):
        return score_tile(image_side, text_side, labels, logit_scale, offset)

    def skipped(unused):
        return (
            jnp.zeros((image_side.shape[0], text_side.shape[0]), jnp.bfloat16),
            jnp.zeros((), jnp.float32),
        )

    return lax.cond(active_flag > 0, active, skipped, 0)


def plain_body(image_emb, text_emb, positives, pair_mask, log_scale, bias):
    reach = (pair_mask.shape[1] - 1) // 2
    block_count = lax.axis_size("blk")
    myself = lax.axis_index("blk")
    logit_scale = jnp.exp(log_scale[0])
    offset = bias[0]
    row_count = image_emb.shape[0]
    image_normed, image_len = unit_rows(image_emb)
    text_normed, text_len = unit_rows(text_emb)
    image_half = image_normed.astype(jnp.bfloat16)
    text_half = text_normed.astype(jnp.bfloat16)
    columns = lax.broadcasted_iota(jnp.int32, (row_count, row_count), 1)
    own_labels = jnp.where(positives[0][:, None] == columns, 1.0, -1.0).astype(jnp.float32)
    apart_labels = -jnp.ones((row_count, row_count), jnp.float32)
    own_flags = lax.dynamic_index_in_dim(pair_mask, myself, 0, keepdims=False)
    fetched = {}
    for direction in (1, -1):
        moving = text_half
        for distance in range(1, reach + 1):
            moving = passed_along(moving, "blk", -direction)
            fetched[direction * distance] = moving
    slopes, loss_sum = masked_tile(
        own_flags[reach], image_half, text_half, own_labels, logit_scale, offset
    )
    image_total = jnp.dot(slopes, text_half, preferred_element_type=jnp.float32)
    text_total = jnp.einsum("rc,rd->cd", slopes, image_half, preferred_element_type=jnp.float32)
    for distance in range(-reach, reach + 1):
        if distance == 0:
            continue
        partner = fetched[distance]
        slopes, part_loss = masked_tile(
            own_flags[reach + distance], image_half, partner, apart_labels, logit_scale, offset
        )
        loss_sum = loss_sum + part_loss
        image_total = image_total + jnp.dot(slopes, partner, preferred_element_type=jnp.float32)
        partial_grad = jnp.einsum(
            "rc,rd->cd", slopes, image_half, preferred_element_type=jnp.float32
        ).astype(jnp.bfloat16)
        arrived = passed_along(partial_grad, "blk", distance)
        text_total = text_total + arrived.astype(jnp.float32)
    total_loss = lax.psum(loss_sum, ("blk", "grp"))
    image_count = row_count * block_count * lax.axis_size("grp")
    loss = (total_loss / image_count).reshape(1)
    image_grad = back_rows(image_normed, image_len, image_total).astype(jnp.bfloat16)
    text_grad = back_rows(text_normed, text_len, text_total).astype(jnp.bfloat16)
    return (image_grad, text_grad, loss)


MESH = pl.DeviceIdType.MESH
Y, INNER, OUTER = 0, 1, 2


def grid_kernel(reach, parts, mask_ref, scale_ref, offset_ref, image_ref, text_ref, pos_row, pos_col,
                image_out, text_out, loss_out,
                got, own, tmp, acc, loss_acc, send_sem, recv_sem):
    me = lax.axis_index("blk")
    grp = lax.axis_index("grp")
    count = lax.axis_size("blk")
    rows = image_ref.shape[0]
    piece = rows // parts
    row, col = me // 2, me % 2
    top = row // 2
    role = row + top * (3 - 2 * row)
    toward = 1 - 2 * top
    aside = row * 2 + (1 - col)
    inner = (row + toward) * 2 + col
    outer = lax.rem((row - toward + 4), 4) * 2 + col
    targets = {Y: aside, INNER: inner, OUTER: outer}
    is_end, is_mid = role == 0, role == 1
    raw = (text_ref, image_ref)

    def block(p, c):
        place = p + top * (3 - 2 * p)
        return place * 2 + col + c * (1 - 2 * col)

    def cut(c):
        return pl.ds(pl.multiple_of(c * piece, piece), piece)

    def remote(way, slot, source, kind, which, c):
        return pltpu.make_async_remote_copy(
            src_ref=source.at[cut(c)], dst_ref=got.at[kind, which, cut(c)],
            send_sem=send_sem.at[way, slot, kind, c], recv_sem=recv_sem.at[kind, which, c],
            device_id=(targets[way], grp), device_id_type=MESH)

    def forward(way, slot, kind, which, c):
        remote(way, slot, got.at[kind, which], kind, which, c).start()

    def arrived(kind, which, c):
        remote(Y, 0, got.at[kind, which], kind, which, c).wait_recv()

    barrier = pltpu.get_barrier_semaphore()
    pl.semaphore_signal(barrier, inc=1, device_id=(aside, grp), device_id_type=MESH)
    pl.semaphore_signal(barrier, inc=1, device_id=(inner, grp), device_id_type=MESH)

    @pl.when(is_mid)
    def _():
        pl.semaphore_signal(barrier, inc=1, device_id=(outer, grp), device_id_type=MESH)
        pl.semaphore_wait(barrier, 3)

    @pl.when(is_end)
    def _():
        pl.semaphore_wait(barrier, 2)

    for kind in (0, 1):
        @pl.loop(0, parts)
        def _(c, kind=kind):
            remote(Y, 0, raw[kind], kind, me, c).start()
            remote(INNER, 0, raw[kind], kind, me, c).start()

            @pl.when(is_mid)
            def _():
                remote(OUTER, 0, raw[kind], kind, me, c).start()

    scale = jnp.exp(scale_ref[...])
    offset = offset_ref[...]

    def normalise(source, target):
        @pl.loop(0, parts)
        def _(c):
            values = source[cut(c), :].astype(jnp.float32)
            length = jnp.sqrt(jnp.sum(values * values, axis=1, keepdims=True) + epsilon)
            target[cut(c), :] = (values / length).astype(jnp.bfloat16)

    def tile(c, side, other):
        similar = lax.dot_general(own[side, cut(c), :], other[...], (((1,), (1,)), ((), ())),
                                  preferred_element_type=jnp.float32)
        return scale * similar + offset

    def flag_of(side, which):
        if side == 0:
            apart = lax.rem(which - me + reach + count, count)
            return mask_ref[me, apart].astype(jnp.float32)
        apart = lax.rem(me - which + reach + count, count)
        return mask_ref[which, apart].astype(jnp.float32)

    def item(side, which):
        normalise(got.at[side, which], tmp)
        flag = flag_of(side, which)

        @pl.loop(0, parts)
        def _(c):
            grown = jnp.exp(tile(c, side, tmp))
            slopes = (grown / (1.0 + grown) * (scale * flag)).astype(jnp.bfloat16)
            acc[side, cut(c), :] += jnp.dot(slopes, tmp[...], preferred_element_type=jnp.float32)
            if side == 0:
                loss_acc[...] += flag * jnp.sum(jnp.log1p(grown), axis=0, keepdims=True)

    def own_item(side):
        @pl.loop(0, parts)
        def _(c):
            logits = tile(c, side, own.at[1 - side])
            flag = mask_ref[me, reach].astype(jnp.float32)
            if side == 0:
                match = pos_col[cut(c), :] == lax.broadcasted_iota(jnp.int32, logits.shape, 1)
            else:
                match = pos_row[...] == lax.broadcasted_iota(jnp.int32, logits.shape, 0) + c * piece
            labels = jnp.where(match, 1.0, -1.0)
            grown = jnp.exp(-labels * logits)
            slopes = (-labels * grown / (1.0 + grown) * (scale * flag)).astype(jnp.bfloat16)
            acc[side, cut(c), :] = jnp.dot(slopes, own[1 - side], preferred_element_type=jnp.float32)
            if side == 0:
                loss_acc[...] += flag * jnp.sum(jnp.log1p(grown), axis=0, keepdims=True)

    loss_acc[...] = jnp.zeros_like(loss_acc)
    normalise(image_ref, own.at[0])
    normalise(text_ref, own.at[1])

    steps = 2 * parts

    @pl.loop(0, steps)
    def _(step):
        kind, c = step // parts, step % parts

        @pl.when(is_mid)
        def _():
            arrived(kind, block(0, 0), c)
            forward(INNER, 1, kind, block(0, 0), c)
            forward(Y, 1, kind, block(0, 0), c)
            arrived(kind, block(2, 0), c)
            arrived(kind, block(1, 1), c)

        @pl.when(is_end)
        def _():
            arrived(kind, block(1, 0), c)
            forward(Y, 1, kind, block(1, 0), c)
            arrived(kind, block(0, 1), c)

        @pl.when(step == 0)
        def _():
            own_item(0)

        @pl.when(step == 1)
        def _():
            own_item(1)

    @pl.when(is_mid)
    def _():
        @pl.loop(0, steps)
        def _(step):
            forward(INNER, 2, step // parts, block(1, 1), step % parts)

    def first_block(i):
        mid_p, mid_c = (2 * i) * (2 - i) + i // 2, i // 2
        end_p, end_c = 1 - i % 2, i % 2
        return block(role * mid_p + (1 - role) * end_p, role * mid_c + (1 - role) * end_c)

    @pl.loop(0, steps)
    def _(step):
        kind, c = step // parts, step % parts
        arrived(kind, block(3, 0), c)
        forward(Y, 2, kind, block(3, 0), c)

        @pl.when(is_mid)
        def _():
            forward(OUTER, 1, kind, block(3, 0), c)

        which = first_block(step // 2)

        @pl.when(step % 2 + 0 * role == 0)
        def _():
            @pl.when(step < 4 + 2 * role)
            def _():
                item(0, which)

        @pl.when(step % 2 == 1)
        def _():
            @pl.when(step < 4 + 2 * role)
            def _():
                item(1, which)

        arrived(kind, block(1 - role, 1), c)

    def second_block(i):
        return block((1 - role) * (3 - 2 * i), (1 - role) * i + role)

    @pl.loop(0, steps)
    def _(step):
        kind, c = step // parts, step % parts
        arrived(kind, block(2, 1), c)

        @pl.when(is_mid)
        def _():
            forward(OUTER, 2, kind, block(2, 1), c)

        late = step // 4
        which = (1 - late) * second_block(step // 2) + late * block(step - 2, 1)
        busy = 1 - (1 - late) * role * (step // 2)

        @pl.when(busy == 1)
        def _():
            @pl.when((1 - late) * (step % 2) == 0)
            def _():
                item(0, which)

            @pl.when((1 - late) * (step % 2) == 1)
            def _():
                item(1, which)

        arrived(kind, block(3, 1), c)

    @pl.loop(2, 4)
    def _(p):
        item(1, block(p, 1))

    for side, source, result in ((0, image_ref, image_out), (1, text_ref, text_out)):
        @pl.loop(0, parts)
        def _(c, side=side, source=source, result=result):
            values = source[cut(c), :].astype(jnp.float32)
            length = jnp.sqrt(jnp.sum(values * values, axis=1, keepdims=True) + epsilon)
            normed = values / length
            result[cut(c), :] = back_rows(normed, length, acc[side, cut(c), :]).astype(result.dtype)

    loss_out[...] = loss_acc[...]

    @pl.loop(0, steps)
    def _(step):
        kind, c = step // parts, step % parts
        for slot in range(3):
            remote(Y, slot, got.at[kind, me], kind, me, c).wait_send()

        remote(INNER, 0, got.at[kind, me], kind, me, c).wait_send()

        @pl.when(is_mid)
        def _():
            remote(INNER, 1, got.at[kind, me], kind, me, c).wait_send()
            remote(INNER, 2, got.at[kind, me], kind, me, c).wait_send()
            for slot in range(3):
                remote(OUTER, slot, got.at[kind, me], kind, me, c).wait_send()


def body(image_emb, text_emb, positives, pair_mask, log_scale, bias):
    reach = (pair_mask.shape[1] - 1) // 2
    block_count = lax.axis_size("blk")
    row_count, width = image_emb.shape
    if block_count != 2 * (reach + 1) or reach != 3 or row_count % (3 * 128) != 0:
        return plain_body(image_emb, text_emb, positives, pair_mask, log_scale, bias)
    parts = 3
    vmem = pl.BlockSpec(memory_space=pltpu.VMEM)
    image_grad, text_grad, losses = pl.pallas_call(
        functools.partial(grid_kernel, reach, parts),
        out_shape=(
            jax.ShapeDtypeStruct(image_emb.shape, image_emb.dtype),
            jax.ShapeDtypeStruct(text_emb.shape, text_emb.dtype),
            jax.ShapeDtypeStruct((1, row_count), jnp.float32),
        ),
        in_specs=[pl.BlockSpec(memory_space=pltpu.SMEM)] + [vmem] * 6,
        out_specs=(vmem,) * 3,
        scratch_shapes=[
            pltpu.VMEM((2, block_count, row_count, width), jnp.bfloat16),
            pltpu.VMEM((2, row_count, width), jnp.bfloat16),
            pltpu.VMEM((row_count, width), jnp.bfloat16),
            pltpu.VMEM((2, row_count, width), jnp.float32),
            pltpu.VMEM((1, row_count), jnp.float32),
            pltpu.SemaphoreType.DMA((3, 3, 2, parts)),
            pltpu.SemaphoreType.DMA((2, block_count, parts)),
        ],
        compiler_params=pltpu.CompilerParams(
            collective_id=0, has_side_effects=True, vmem_limit_bytes=48 * 1024 * 1024
        ),
    )(pair_mask, log_scale.reshape(1, 1), bias.reshape(1, 1), image_emb, text_emb, positives,
      positives.reshape(row_count, 1))
    total_loss = lax.psum(jnp.sum(losses), ("blk", "grp"))
    image_count = row_count * block_count * lax.axis_size("grp")
    return (image_grad, text_grad, (total_loss / image_count).reshape(1))


def solution(mesh):
    return jax.shard_map(
        body,
        mesh=mesh,
        in_specs=(
            P(("blk", "grp"), None),
            P(("blk", "grp"), None),
            P(("blk", "grp"), None),
            P(),
            P(),
            P(),
        ),
        out_specs=(P(("blk", "grp"), None), P(("blk", "grp"), None), P()),
        check_vma=False,
    )
```

```python
import functools

import jax
import jax.numpy as jnp
from jax import lax
from jax.experimental import pallas as pl
from jax.experimental.pallas import tpu as pltpu
from jax.sharding import PartitionSpec as P

epsilon = 1e-06


def passed_along(value, axis, steps):
    count = lax.axis_size(axis)
    pairs = [(source, (source + steps) % count) for source in range(count)]
    return lax.ppermute(value, axis, pairs)


def unit_rows(embedded):
    values = embedded.astype(jnp.float32)
    length = jnp.sqrt(jnp.sum(values * values, axis=1, keepdims=True) + epsilon)
    return (values / length, length)


def back_rows(normed, length, upstream):
    inward = jnp.sum(normed * upstream, axis=1, keepdims=True)
    return (upstream - normed * inward) / length


def score_tile(image_side, text_side, labels, logit_scale, offset):
    similar = jnp.einsum("rd,cd->rc", image_side, text_side, preferred_element_type=jnp.float32)
    logits = logit_scale * similar + offset
    signed = labels * logits
    loss_sum = jnp.sum(jax.nn.softplus(-signed))
    slopes = (-labels * jax.nn.sigmoid(-signed) * logit_scale).astype(jnp.bfloat16)
    return (slopes, loss_sum)


def masked_tile(active_flag, image_side, text_side, labels, logit_scale, offset):

    def active(unused):
        return score_tile(image_side, text_side, labels, logit_scale, offset)

    def skipped(unused):
        return (
            jnp.zeros((image_side.shape[0], text_side.shape[0]), jnp.bfloat16),
            jnp.zeros((), jnp.float32),
        )

    return lax.cond(active_flag > 0, active, skipped, 0)


def plain_body(image_emb, text_emb, positives, pair_mask, log_scale, bias):
    reach = (pair_mask.shape[1] - 1) // 2
    block_count = lax.axis_size("blk")
    myself = lax.axis_index("blk")
    logit_scale = jnp.exp(log_scale[0])
    offset = bias[0]
    row_count = image_emb.shape[0]
    image_normed, image_len = unit_rows(image_emb)
    text_normed, text_len = unit_rows(text_emb)
    image_half = image_normed.astype(jnp.bfloat16)
    text_half = text_normed.astype(jnp.bfloat16)
    columns = lax.broadcasted_iota(jnp.int32, (row_count, row_count), 1)
    own_labels = jnp.where(positives[0][:, None] == columns, 1.0, -1.0).astype(jnp.float32)
    apart_labels = -jnp.ones((row_count, row_count), jnp.float32)
    own_flags = lax.dynamic_index_in_dim(pair_mask, myself, 0, keepdims=False)
    fetched = {}
    for direction in (1, -1):
        moving = text_half
        for distance in range(1, reach + 1):
            moving = passed_along(moving, "blk", -direction)
            fetched[direction * distance] = moving
    slopes, loss_sum = masked_tile(
        own_flags[reach], image_half, text_half, own_labels, logit_scale, offset
    )
    image_total = jnp.dot(slopes, text_half, preferred_element_type=jnp.float32)
    text_total = jnp.einsum("rc,rd->cd", slopes, image_half, preferred_element_type=jnp.float32)
    for distance in range(-reach, reach + 1):
        if distance == 0:
            continue
        partner = fetched[distance]
        slopes, part_loss = masked_tile(
            own_flags[reach + distance], image_half, partner, apart_labels, logit_scale, offset
        )
        loss_sum = loss_sum + part_loss
        image_total = image_total + jnp.dot(slopes, partner, preferred_element_type=jnp.float32)
        partial_grad = jnp.einsum(
            "rc,rd->cd", slopes, image_half, preferred_element_type=jnp.float32
        ).astype(jnp.bfloat16)
        arrived = passed_along(partial_grad, "blk", distance)
        text_total = text_total + arrived.astype(jnp.float32)
    total_loss = lax.psum(loss_sum, ("blk", "grp"))
    image_count = row_count * block_count * lax.axis_size("grp")
    loss = (total_loss / image_count).reshape(1)
    image_grad = back_rows(image_normed, image_len, image_total).astype(jnp.bfloat16)
    text_grad = back_rows(text_normed, text_len, text_total).astype(jnp.bfloat16)
    return (image_grad, text_grad, loss)


MESH = pl.DeviceIdType.MESH
Y, INNER, OUTER = 0, 1, 2


def grid_kernel(reach, parts, tiles, mask_ref, scale_ref, offset_ref, image_hbm, text_hbm, pos_row, pos_col,
                image_out, text_out, loss_out,
                held, got, own, tmp, acc, loss_acc, blk_loss, grp_loss,
                load_sem, send_sem, recv_sem, blk_send, blk_recv, grp_send, grp_recv):
    me = lax.axis_index("blk")
    grp = lax.axis_index("grp")
    count = lax.axis_size("blk")
    groups = lax.axis_size("grp")
    rows = held.shape[1]
    piece = rows // parts
    tall = rows // tiles
    image_ref, text_ref = held.at[1], held.at[0]
    row, col = me // 2, me % 2
    top = row // 2
    role = row + top * (3 - 2 * row)
    toward = 1 - 2 * top
    aside = row * 2 + (1 - col)
    inner = (row + toward) * 2 + col
    outer = lax.rem((row - toward + 4), 4) * 2 + col
    targets = {Y: aside, INNER: inner, OUTER: outer}
    is_end, is_mid = role == 0, role == 1
    raw = (text_ref, image_ref)

    def block(p, c):
        place = p + top * (3 - 2 * p)
        return place * 2 + col + c * (1 - 2 * col)

    def cut(c):
        return pl.ds(pl.multiple_of(c * piece, piece), piece)

    def band(c):
        return pl.ds(pl.multiple_of(c * tall, tall), tall)

    def remote(way, slot, source, kind, which, c):
        return pltpu.make_async_remote_copy(
            src_ref=source.at[cut(c)], dst_ref=got.at[kind, which, cut(c)],
            send_sem=send_sem.at[way, slot, kind, c], recv_sem=recv_sem.at[kind, which, c],
            device_id=(targets[way], grp), device_id_type=MESH)

    def forward(way, slot, kind, which, c):
        remote(way, slot, got.at[kind, which], kind, which, c).start()

    def arrived(kind, which, c):
        remote(Y, 0, got.at[kind, which], kind, which, c).wait_recv()

    loads = [
        pltpu.make_async_copy(source, held.at[kind], load_sem.at[kind])
        for kind, source in ((0, text_hbm), (1, image_hbm))
    ]
    for load in loads:
        load.start()
    barrier = pltpu.get_barrier_semaphore()

    @pl.loop(1, count)
    def _(d):
        pl.semaphore_signal(barrier, inc=1, device_id=(lax.rem(me + d, count), grp), device_id_type=MESH)

    @pl.loop(1, groups)
    def _(d):
        pl.semaphore_signal(barrier, inc=1, device_id=(me, lax.rem(grp + d, groups)), device_id_type=MESH)

    pl.semaphore_wait(barrier, count + groups - 2)

    def blk_share(d):
        target = lax.rem(me + d, count)
        return pltpu.make_async_remote_copy(
            src_ref=blk_loss.at[me], dst_ref=blk_loss.at[me], send_sem=blk_send.at[d],
            recv_sem=blk_recv.at[me], device_id=(target, grp), device_id_type=MESH)

    def blk_arrival(d):
        source = lax.rem(me + d, count)
        return pltpu.make_async_remote_copy(
            src_ref=blk_loss.at[source], dst_ref=blk_loss.at[source], send_sem=blk_send.at[d],
            recv_sem=blk_recv.at[source], device_id=(source, grp), device_id_type=MESH)

    def grp_share(d):
        target = lax.rem(grp + d, groups)
        return pltpu.make_async_remote_copy(
            src_ref=grp_loss.at[grp], dst_ref=grp_loss.at[grp], send_sem=grp_send.at[d],
            recv_sem=grp_recv.at[grp], device_id=(me, target), device_id_type=MESH)

    def grp_arrival(d):
        source = lax.rem(grp + d, groups)
        return pltpu.make_async_remote_copy(
            src_ref=grp_loss.at[source], dst_ref=grp_loss.at[source], send_sem=grp_send.at[d],
            recv_sem=grp_recv.at[source], device_id=(me, source), device_id_type=MESH)

    for kind in (0, 1):
        loads[kind].wait()

        @pl.loop(0, parts)
        def _(c, kind=kind):
            remote(Y, 0, raw[kind], kind, me, c).start()
            remote(INNER, 0, raw[kind], kind, me, c).start()

            @pl.when(is_mid)
            def _():
                remote(OUTER, 0, raw[kind], kind, me, c).start()

    scale = jnp.exp(jnp.full((1, 1), scale_ref[0], jnp.float32))
    offset = jnp.full((1, 1), offset_ref[0], jnp.float32)

    def normalise(source, target):
        @pl.loop(0, tiles)
        def _(c):
            values = source[band(c), :].astype(jnp.float32)
            length = jnp.sqrt(jnp.sum(values * values, axis=1, keepdims=True) + epsilon)
            target[band(c), :] = (values / length).astype(jnp.bfloat16)

    def tile(c, side, other):
        similar = lax.dot_general(own[side, band(c), :], other[...], (((1,), (1,)), ((), ())),
                                  preferred_element_type=jnp.float32)
        return scale * similar + offset

    def flag_of(side, which):
        if side == 0:
            apart = lax.rem(which - me + reach + count, count)
            return mask_ref[me, apart].astype(jnp.float32)
        apart = lax.rem(me - which + reach + count, count)
        return mask_ref[which, apart].astype(jnp.float32)

    def item(side, which):
        normalise(got.at[side, which], tmp)
        flag = flag_of(side, which)

        @pl.loop(0, tiles)
        def _(c):
            grown = jnp.exp(tile(c, side, tmp))
            slopes = (grown / (1.0 + grown) * (scale * flag)).astype(jnp.bfloat16)
            acc[side, band(c), :] += jnp.dot(slopes, tmp[...], preferred_element_type=jnp.float32)
            if side == 0:
                loss_acc[...] += flag * jnp.sum(jnp.log1p(grown), axis=0, keepdims=True)

    def own_item(side):
        @pl.loop(0, tiles)
        def _(c):
            logits = tile(c, side, own.at[1 - side])
            flag = mask_ref[me, reach].astype(jnp.float32)
            if side == 0:
                match = pos_col[band(c), :] == lax.broadcasted_iota(jnp.int32, logits.shape, 1)
            else:
                match = pos_row[...] == lax.broadcasted_iota(jnp.int32, logits.shape, 0) + c * tall
            labels = jnp.where(match, 1.0, -1.0)
            grown = jnp.exp(-labels * logits)
            slopes = (-labels * grown / (1.0 + grown) * (scale * flag)).astype(jnp.bfloat16)
            acc[side, band(c), :] = jnp.dot(slopes, own[1 - side], preferred_element_type=jnp.float32)
            if side == 0:
                loss_acc[...] += flag * jnp.sum(jnp.log1p(grown), axis=0, keepdims=True)

    def short_item(which, k):
        values = got[1, which, band(k), :].astype(jnp.float32)
        length = jnp.sqrt(jnp.sum(values * values, axis=1, keepdims=True) + epsilon)
        tmp[0:tall, :] = (values / length).astype(jnp.bfloat16)
        flag = flag_of(1, which)

        @pl.loop(0, tiles)
        def _(c):
            grown = jnp.exp(tile(c, 1, tmp.at[0:tall]))
            slopes = (grown / (1.0 + grown) * (scale * flag)).astype(jnp.bfloat16)
            acc[1, band(c), :] += jnp.dot(slopes, tmp[0:tall, :], preferred_element_type=jnp.float32)

    def finish(side, source, result):
        @pl.loop(0, tiles)
        def _(c):
            values = source[band(c), :].astype(jnp.float32)
            length = jnp.sqrt(jnp.sum(values * values, axis=1, keepdims=True) + epsilon)
            normed = values / length
            result[band(c), :] = back_rows(normed, length, acc[side, band(c), :]).astype(result.dtype)

    loss_acc[...] = jnp.zeros_like(loss_acc)
    normalise(image_ref, own.at[0])
    normalise(text_ref, own.at[1])

    steps = 2 * parts

    @pl.loop(0, steps)
    def _(step):
        kind, c = step // parts, step % parts

        @pl.when(is_mid)
        def _():
            arrived(kind, block(0, 0), c)
            forward(INNER, 1, kind, block(0, 0), c)
            forward(Y, 1, kind, block(0, 0), c)
            arrived(kind, block(2, 0), c)
            arrived(kind, block(1, 1), c)

        @pl.when(is_end)
        def _():
            arrived(kind, block(1, 0), c)
            forward(Y, 1, kind, block(1, 0), c)
            arrived(kind, block(0, 1), c)

        @pl.when(step == 0)
        def _():
            own_item(0)

        @pl.when(step == 1)
        def _():
            own_item(1)

    @pl.when(is_mid)
    def _():
        @pl.loop(0, steps)
        def _(step):
            forward(INNER, 2, step // parts, block(1, 1), step % parts)

    def first_block(i):
        mid_p, mid_c = (2 * i) * (2 - i) + i // 2, i // 2
        end_p, end_c = 1 - i % 2, i % 2
        return block(role * mid_p + (1 - role) * end_p, role * mid_c + (1 - role) * end_c)

    @pl.loop(0, steps)
    def _(step):
        kind, c = step // parts, step % parts
        arrived(kind, block(3, 0), c)
        forward(Y, 2, kind, block(3, 0), c)

        @pl.when(is_mid)
        def _():
            forward(OUTER, 1, kind, block(3, 0), c)

        which = first_block(step // 4)
        wanted = (1 - step % 2) * (role + (1 - role) * (1 - step // 8))

        @pl.when(wanted * (2 - step // 2 % 2) == 2)
        def _():
            item(0, which)

        @pl.when(wanted * (1 + step // 2 % 2) == 2)
        def _():
            item(1, which)

        arrived(kind, block(1 - role, 1), c)

    def second_block(i):
        return block((1 - role) * (3 - 2 * i), (1 - role) * i + role)

    @pl.loop(0, steps)
    def _(step):
        kind, c = step // parts, step % parts
        arrived(kind, block(2, 1), c)

        @pl.when(is_mid)
        def _():
            forward(OUTER, 2, kind, block(2, 1), c)

        wanted = (1 - (step + 8) // 12) * (1 - role * (step // 2))

        @pl.when(wanted * (2 - step % 2) == 2)
        def _():
            item(0, second_block(step // 2))

        @pl.when(wanted * (1 + step % 2) == 2)
        def _():
            item(1, second_block(step // 2))

        @pl.when(step == parts)
        def _():
            item(0, block(2, 1))

        arrived(kind, block(3, 1), c)

        @pl.when(step == parts + 1)
        def _():
            item(0, block(3, 1))
            blk_loss[me] = jnp.full(blk_loss.shape[1:], jnp.sum(loss_acc[...]), jnp.float32)

        @pl.when(step == parts + 2)
        def _():
            finish(0, image_ref, image_out)

            @pl.loop(1, count)
            def _(d):
                blk_share(d).start()

        @pl.when(step == parts + 3)
        def _():
            short_item(block(2, 1), 0)
            short_item(block(3, 1), 0)

        @pl.when(step == parts + 4)
        def _():
            short_item(block(2, 1), 1)
            short_item(block(3, 1), 1)

    @pl.loop(1, count)
    def _(d):
        blk_arrival(d).wait_recv()

    grp_loss[grp] = jnp.sum(blk_loss[...], axis=0)
    short_item(block(2, 1), 2)

    @pl.loop(1, groups)
    def _(d):
        grp_share(d).start()

    short_item(block(3, 1), 2)
    finish(1, text_ref, text_out)

    @pl.loop(1, groups)
    def _(d):
        grp_arrival(d).wait_recv()

    total = jnp.sum(grp_loss[...], axis=0)
    loss_out[0] = jnp.sum(total[0:1, 0:1]) / (rows * count * groups)

    @pl.loop(1, count)
    def _(d):
        blk_share(d).wait_send()

    @pl.loop(1, groups)
    def _(d):
        grp_share(d).wait_send()

    @pl.loop(0, steps)
    def _(step):
        kind, c = step // parts, step % parts
        for slot in range(3):
            remote(Y, slot, got.at[kind, me], kind, me, c).wait_send()

        remote(INNER, 0, got.at[kind, me], kind, me, c).wait_send()

        @pl.when(is_mid)
        def _():
            remote(INNER, 1, got.at[kind, me], kind, me, c).wait_send()
            remote(INNER, 2, got.at[kind, me], kind, me, c).wait_send()
            for slot in range(3):
                remote(OUTER, slot, got.at[kind, me], kind, me, c).wait_send()


def body(image_emb, text_emb, positives, pair_mask, log_scale, bias):
    reach = (pair_mask.shape[1] - 1) // 2
    block_count = lax.axis_size("blk")
    row_count, width = image_emb.shape
    if block_count != 2 * (reach + 1) or reach != 3 or row_count % (3 * 128) != 0:
        return plain_body(image_emb, text_emb, positives, pair_mask, log_scale, bias)
    parts, tiles = 6, 3
    groups = lax.axis_size("grp")
    vmem = pl.BlockSpec(memory_space=pltpu.VMEM)
    smem = pl.BlockSpec(memory_space=pltpu.SMEM)
    anywhere = pl.BlockSpec(memory_space=pl.ANY)
    return pl.pallas_call(
        functools.partial(grid_kernel, reach, parts, tiles),
        out_shape=(
            jax.ShapeDtypeStruct(image_emb.shape, image_emb.dtype),
            jax.ShapeDtypeStruct(text_emb.shape, text_emb.dtype),
            jax.ShapeDtypeStruct((1,), jnp.float32),
        ),
        in_specs=[smem] * 3 + [anywhere] * 2 + [vmem] * 2,
        out_specs=(vmem, vmem, smem),
        scratch_shapes=[
            pltpu.VMEM((2, row_count, width), jnp.bfloat16),
            pltpu.VMEM((2, block_count, row_count, width), jnp.bfloat16),
            pltpu.VMEM((2, row_count, width), jnp.bfloat16),
            pltpu.VMEM((row_count, width), jnp.bfloat16),
            pltpu.VMEM((2, row_count, width), jnp.float32),
            pltpu.VMEM((1, row_count), jnp.float32),
            pltpu.VMEM((block_count, 8, 128), jnp.float32),
            pltpu.VMEM((groups, 8, 128), jnp.float32),
            pltpu.SemaphoreType.DMA((2,)),
            pltpu.SemaphoreType.DMA((3, 3, 2, parts)),
            pltpu.SemaphoreType.DMA((2, block_count, parts)),
            pltpu.SemaphoreType.DMA((block_count,)),
            pltpu.SemaphoreType.DMA((block_count,)),
            pltpu.SemaphoreType.DMA((groups,)),
            pltpu.SemaphoreType.DMA((groups,)),
        ],
        compiler_params=pltpu.CompilerParams(
            collective_id=0, has_side_effects=True, vmem_limit_bytes=56 * 1024 * 1024
        ),
    )(pair_mask, log_scale, bias, image_emb, text_emb, positives, positives.reshape(row_count, 1))


def solution(mesh):
    return jax.shard_map(
        body,
        mesh=mesh,
        in_specs=(
            P(("blk", "grp"), None),
            P(("blk", "grp"), None),
            P(("blk", "grp"), None),
            P(),
            P(),
            P(),
        ),
        out_specs=(P(("blk", "grp"), None), P(("blk", "grp"), None), P()),
        check_vma=False,
    )
```

```python
import functools

import jax
import jax.numpy as jnp
from jax import lax
from jax.experimental import pallas as pl
from jax.experimental.pallas import tpu as pltpu
from jax.sharding import PartitionSpec as P

epsilon = 1e-06


def passed_along(value, axis, steps):
    count = lax.axis_size(axis)
    pairs = [(source, (source + steps) % count) for source in range(count)]
    return lax.ppermute(value, axis, pairs)


def unit_rows(embedded):
    values = embedded.astype(jnp.float32)
    length = jnp.sqrt(jnp.sum(values * values, axis=1, keepdims=True) + epsilon)
    return (values / length, length)


def back_rows(normed, length, upstream):
    inward = jnp.sum(normed * upstream, axis=1, keepdims=True)
    return (upstream - normed * inward) / length


def score_tile(image_side, text_side, labels, logit_scale, offset):
    similar = jnp.einsum("rd,cd->rc", image_side, text_side, preferred_element_type=jnp.float32)
    logits = logit_scale * similar + offset
    signed = labels * logits
    loss_sum = jnp.sum(jax.nn.softplus(-signed))
    slopes = (-labels * jax.nn.sigmoid(-signed) * logit_scale).astype(jnp.bfloat16)
    return (slopes, loss_sum)


def masked_tile(active_flag, image_side, text_side, labels, logit_scale, offset):

    def active(unused):
        return score_tile(image_side, text_side, labels, logit_scale, offset)

    def skipped(unused):
        return (
            jnp.zeros((image_side.shape[0], text_side.shape[0]), jnp.bfloat16),
            jnp.zeros((), jnp.float32),
        )

    return lax.cond(active_flag > 0, active, skipped, 0)


def plain_body(image_emb, text_emb, positives, pair_mask, log_scale, bias):
    reach = (pair_mask.shape[1] - 1) // 2
    block_count = lax.axis_size("blk")
    myself = lax.axis_index("blk")
    logit_scale = jnp.exp(log_scale[0])
    offset = bias[0]
    row_count = image_emb.shape[0]
    image_normed, image_len = unit_rows(image_emb)
    text_normed, text_len = unit_rows(text_emb)
    image_half = image_normed.astype(jnp.bfloat16)
    text_half = text_normed.astype(jnp.bfloat16)
    columns = lax.broadcasted_iota(jnp.int32, (row_count, row_count), 1)
    own_labels = jnp.where(positives[0][:, None] == columns, 1.0, -1.0).astype(jnp.float32)
    apart_labels = -jnp.ones((row_count, row_count), jnp.float32)
    own_flags = lax.dynamic_index_in_dim(pair_mask, myself, 0, keepdims=False)
    fetched = {}
    for direction in (1, -1):
        moving = text_half
        for distance in range(1, reach + 1):
            moving = passed_along(moving, "blk", -direction)
            fetched[direction * distance] = moving
    slopes, loss_sum = masked_tile(
        own_flags[reach], image_half, text_half, own_labels, logit_scale, offset
    )
    image_total = jnp.dot(slopes, text_half, preferred_element_type=jnp.float32)
    text_total = jnp.einsum("rc,rd->cd", slopes, image_half, preferred_element_type=jnp.float32)
    for distance in range(-reach, reach + 1):
        if distance == 0:
            continue
        partner = fetched[distance]
        slopes, part_loss = masked_tile(
            own_flags[reach + distance], image_half, partner, apart_labels, logit_scale, offset
        )
        loss_sum = loss_sum + part_loss
        image_total = image_total + jnp.dot(slopes, partner, preferred_element_type=jnp.float32)
        partial_grad = jnp.einsum(
            "rc,rd->cd", slopes, image_half, preferred_element_type=jnp.float32
        ).astype(jnp.bfloat16)
        arrived = passed_along(partial_grad, "blk", distance)
        text_total = text_total + arrived.astype(jnp.float32)
    total_loss = lax.psum(loss_sum, ("blk", "grp"))
    image_count = row_count * block_count * lax.axis_size("grp")
    loss = (total_loss / image_count).reshape(1)
    image_grad = back_rows(image_normed, image_len, image_total).astype(jnp.bfloat16)
    text_grad = back_rows(text_normed, text_len, text_total).astype(jnp.bfloat16)
    return (image_grad, text_grad, loss)


MESH = pl.DeviceIdType.MESH
Y, INNER, OUTER = 0, 1, 2


def grid_kernel(reach, parts, tiles, mask_ref, scale_ref, offset_ref, image_hbm, text_hbm, pos_hbm,
                image_out, text_out, loss_out,
                held, pos_row, ready, got, own, tmp, acc, loss_acc, blk_loss, grp_loss,
                load_sem, out_sem, send_sem, recv_sem, blk_send, blk_recv, grp_send, grp_recv):
    me = lax.axis_index("blk")
    grp = lax.axis_index("grp")
    count = lax.axis_size("blk")
    groups = lax.axis_size("grp")
    rows = held.shape[1]
    piece = rows // parts
    tall = rows // tiles
    image_ref, text_ref = held.at[1], held.at[0]
    row, col = me // 2, me % 2
    top = row // 2
    role = row + top * (3 - 2 * row)
    toward = 1 - 2 * top
    aside = row * 2 + (1 - col)
    inner = (row + toward) * 2 + col
    outer = lax.rem((row - toward + 4), 4) * 2 + col
    targets = {Y: aside, INNER: inner, OUTER: outer}
    is_end, is_mid = role == 0, role == 1
    raw = (text_ref, image_ref)

    def block(p, c):
        place = p + top * (3 - 2 * p)
        return place * 2 + col + c * (1 - 2 * col)

    def cut(c):
        return pl.ds(pl.multiple_of(c * piece, piece), piece)

    def band(c):
        return pl.ds(pl.multiple_of(c * tall, tall), tall)

    def remote(way, slot, source, kind, which, c):
        return pltpu.make_async_remote_copy(
            src_ref=source.at[cut(c)], dst_ref=got.at[kind, which, cut(c)],
            send_sem=send_sem.at[way, slot, kind, c], recv_sem=recv_sem.at[kind, which, c],
            device_id=(targets[way], grp), device_id_type=MESH)

    def forward(way, slot, kind, which, c):
        remote(way, slot, got.at[kind, which], kind, which, c).start()

    def arrived(kind, which, c):
        remote(Y, 0, got.at[kind, which], kind, which, c).wait_recv()

    loads = [
        pltpu.make_async_copy(source, held.at[kind], load_sem.at[kind])
        for kind, source in ((0, text_hbm), (1, image_hbm))
    ]
    loads.append(pltpu.make_async_copy(pos_hbm, pos_row, load_sem.at[2]))
    for load in loads:
        load.start()
    barrier = pltpu.get_barrier_semaphore()

    @pl.loop(1, count)
    def _(d):
        pl.semaphore_signal(barrier, inc=1, device_id=(lax.rem(me + d, count), grp), device_id_type=MESH)

    @pl.loop(1, groups)
    def _(d):
        pl.semaphore_signal(barrier, inc=1, device_id=(me, lax.rem(grp + d, groups)), device_id_type=MESH)

    pl.semaphore_wait(barrier, count + groups - 2)

    def blk_share(d):
        target = lax.rem(me + d, count)
        return pltpu.make_async_remote_copy(
            src_ref=blk_loss.at[me], dst_ref=blk_loss.at[me], send_sem=blk_send.at[d],
            recv_sem=blk_recv.at[me], device_id=(target, grp), device_id_type=MESH)

    def blk_arrival(d):
        source = lax.rem(me + d, count)
        return pltpu.make_async_remote_copy(
            src_ref=blk_loss.at[source], dst_ref=blk_loss.at[source], send_sem=blk_send.at[d],
            recv_sem=blk_recv.at[source], device_id=(source, grp), device_id_type=MESH)

    def grp_share(d):
        target = lax.rem(grp + d, groups)
        return pltpu.make_async_remote_copy(
            src_ref=grp_loss.at[grp], dst_ref=grp_loss.at[grp], send_sem=grp_send.at[d],
            recv_sem=grp_recv.at[grp], device_id=(me, target), device_id_type=MESH)

    def grp_arrival(d):
        source = lax.rem(grp + d, groups)
        return pltpu.make_async_remote_copy(
            src_ref=grp_loss.at[source], dst_ref=grp_loss.at[source], send_sem=grp_send.at[d],
            recv_sem=grp_recv.at[source], device_id=(me, source), device_id_type=MESH)

    for kind in (0, 1):
        loads[kind].wait()

        @pl.loop(0, parts)
        def _(c, kind=kind):
            remote(Y, 0, raw[kind], kind, me, c).start()
            remote(INNER, 0, raw[kind], kind, me, c).start()

            @pl.when(is_mid)
            def _():
                remote(OUTER, 0, raw[kind], kind, me, c).start()

    scale = jnp.exp(jnp.full((1, 1), scale_ref[0], jnp.float32))
    offset = jnp.full((1, 1), offset_ref[0], jnp.float32)

    def normalise(source, target):
        @pl.loop(0, tiles)
        def _(c):
            values = source[band(c), :].astype(jnp.float32)
            length = jnp.sqrt(jnp.sum(values * values, axis=1, keepdims=True) + epsilon)
            target[band(c), :] = (values / length).astype(jnp.bfloat16)

    def tile(c, side, other):
        similar = lax.dot_general(own[side, band(c), :], other[...], (((1,), (1,)), ((), ())),
                                  preferred_element_type=jnp.float32)
        return scale * similar + offset

    def flag_of(side, which):
        if side == 0:
            apart = lax.rem(which - me + reach + count, count)
            return mask_ref[me, apart].astype(jnp.float32)
        apart = lax.rem(me - which + reach + count, count)
        return mask_ref[which, apart].astype(jnp.float32)

    def item(side, which):
        normalise(got.at[side, which], tmp)
        flag = flag_of(side, which)

        @pl.loop(0, tiles)
        def _(c):
            grown = jnp.exp(tile(c, side, tmp))
            slopes = (grown / (1.0 + grown) * (scale * flag)).astype(jnp.bfloat16)
            acc[side, band(c), :] += jnp.dot(slopes, tmp[...], preferred_element_type=jnp.float32)
            if side == 0:
                loss_acc[...] += flag * jnp.sum(jnp.log1p(grown), axis=0, keepdims=True)

    def own_item(side):
        @pl.loop(0, tiles)
        def _(c):
            logits = tile(c, side, own.at[1 - side])
            flag = mask_ref[me, reach].astype(jnp.float32)
            if side == 0:
                hit = pos_row[:, band(c)] == lax.broadcasted_iota(jnp.int32, (rows, tall), 0)
                labels = jnp.transpose(jnp.where(hit, 1.0, -1.0))
            else:
                hit = pos_row[...] == lax.broadcasted_iota(jnp.int32, logits.shape, 0) + c * tall
                labels = jnp.where(hit, 1.0, -1.0)
            grown = jnp.exp(-labels * logits)
            slopes = (-labels * grown / (1.0 + grown) * (scale * flag)).astype(jnp.bfloat16)
            acc[side, band(c), :] = jnp.dot(slopes, own[1 - side], preferred_element_type=jnp.float32)
            if side == 0:
                loss_acc[...] += flag * jnp.sum(jnp.log1p(grown), axis=0, keepdims=True)

    def short_item(which, k):
        values = got[1, which, band(k), :].astype(jnp.float32)
        length = jnp.sqrt(jnp.sum(values * values, axis=1, keepdims=True) + epsilon)
        tmp[0:tall, :] = (values / length).astype(jnp.bfloat16)
        flag = flag_of(1, which)

        @pl.loop(0, tiles)
        def _(c):
            grown = jnp.exp(tile(c, 1, tmp.at[0:tall]))
            slopes = (grown / (1.0 + grown) * (scale * flag)).astype(jnp.bfloat16)
            acc[1, band(c), :] += jnp.dot(slopes, tmp[0:tall, :], preferred_element_type=jnp.float32)

    def put_out(side, result, c):
        return pltpu.make_async_copy(ready.at[side, band(c)], result.at[band(c)], out_sem.at[side, c])

    def finish(side, source, result):
        @pl.loop(0, tiles)
        def _(c):
            values = source[band(c), :].astype(jnp.float32)
            length = jnp.sqrt(jnp.sum(values * values, axis=1, keepdims=True) + epsilon)
            normed = values / length
            ready[side, band(c), :] = back_rows(normed, length, acc[side, band(c), :]).astype(ready.dtype)
            put_out(side, result, c).start()

    loads[2].wait()
    loss_acc[...] = jnp.zeros_like(loss_acc)
    normalise(image_ref, own.at[0])
    normalise(text_ref, own.at[1])

    steps = 2 * parts

    @pl.loop(0, steps)
    def _(step):
        kind, c = step // parts, step % parts

        @pl.when(is_mid)
        def _():
            arrived(kind, block(0, 0), c)
            forward(INNER, 1, kind, block(0, 0), c)
            forward(Y, 1, kind, block(0, 0), c)
            arrived(kind, block(2, 0), c)
            arrived(kind, block(1, 1), c)

        @pl.when(is_end)
        def _():
            arrived(kind, block(1, 0), c)
            forward(Y, 1, kind, block(1, 0), c)
            arrived(kind, block(0, 1), c)

        @pl.when(step == 0)
        def _():
            own_item(0)

        @pl.when(step == 1)
        def _():
            own_item(1)

    @pl.when(is_mid)
    def _():
        @pl.loop(0, steps)
        def _(step):
            forward(INNER, 2, step // parts, block(1, 1), step % parts)

    def first_block(i):
        mid_p, mid_c = (2 * i) * (2 - i) + i // 2, i // 2
        end_p, end_c = 1 - i % 2, i % 2
        return block(role * mid_p + (1 - role) * end_p, role * mid_c + (1 - role) * end_c)

    @pl.loop(0, steps)
    def _(step):
        kind, c = step // parts, step % parts
        arrived(kind, block(3, 0), c)
        forward(Y, 2, kind, block(3, 0), c)

        @pl.when(is_mid)
        def _():
            forward(OUTER, 1, kind, block(3, 0), c)

        which = first_block(step // 4)
        wanted = (1 - step % 2) * (role + (1 - role) * (1 - step // 8))

        @pl.when(wanted * (2 - step // 2 % 2) == 2)
        def _():
            item(0, which)

        @pl.when(wanted * (1 + step // 2 % 2) == 2)
        def _():
            item(1, which)

        arrived(kind, block(1 - role, 1), c)

    def second_block(i):
        return block((1 - role) * (3 - 2 * i), (1 - role) * i + role)

    @pl.loop(0, steps - 1)
    def _(step):
        kind, c = step // parts, step % parts
        arrived(kind, block(2, 1), c)

        @pl.when(is_mid)
        def _():
            forward(OUTER, 2, kind, block(2, 1), c)

        wanted = (1 - (step + 8) // 12) * (1 - role * (step // 2))

        @pl.when(wanted * (2 - step % 2) == 2)
        def _():
            item(0, second_block(step // 2))

        @pl.when(wanted * (1 + step % 2) == 2)
        def _():
            item(1, second_block(step // 2))

        @pl.when(step == parts)
        def _():
            item(0, block(2, 1))

        arrived(kind, block(3, 1), c)

        @pl.when(step == parts + 1)
        def _():
            item(0, block(3, 1))
            blk_loss[me] = jnp.full(blk_loss.shape[1:], jnp.sum(loss_acc[...]), jnp.float32)

        @pl.when(step == parts + 2)
        def _():
            finish(0, image_ref, image_out)

            @pl.loop(1, count)
            def _(d):
                blk_share(d).start()

        @pl.when(step == parts + 3)
        def _():
            short_item(block(2, 1), 0)
            short_item(block(3, 1), 0)

        @pl.when(step == parts + 4)
        def _():
            short_item(block(2, 1), 1)
            short_item(block(3, 1), 1)

    final = role * 0 + parts - 1

    @pl.when(is_mid)
    def _():
        arrived(1, block(2, 1), final)
        forward(OUTER, 2, 1, block(2, 1), final)

    arrived(1, block(3, 1), final)

    @pl.loop(1, count)
    def _(d):
        blk_arrival(d).wait_recv()

    grp_loss[grp] = jnp.sum(blk_loss[...], axis=0)
    short_item(block(3, 1), 2)

    @pl.loop(1, groups)
    def _(d):
        grp_share(d).start()

    @pl.when(is_end)
    def _():
        arrived(1, block(2, 1), final)

    short_item(block(2, 1), 2)
    finish(1, text_ref, text_out)

    @pl.loop(1, groups)
    def _(d):
        grp_arrival(d).wait_recv()

    total = jnp.sum(grp_loss[...], axis=0)
    @pl.loop(0, tiles)
    def _(c):
        put_out(0, image_out, c).wait()
        put_out(1, text_out, c).wait()

    loss_out[0] = jnp.sum(total[0:1, 0:1]) / (rows * count * groups)

    @pl.loop(1, count)
    def _(d):
        blk_share(d).wait_send()

    @pl.loop(1, groups)
    def _(d):
        grp_share(d).wait_send()

    @pl.loop(0, steps)
    def _(step):
        kind, c = step // parts, step % parts
        for slot in range(3):
            remote(Y, slot, got.at[kind, me], kind, me, c).wait_send()

        remote(INNER, 0, got.at[kind, me], kind, me, c).wait_send()

        @pl.when(is_mid)
        def _():
            remote(INNER, 1, got.at[kind, me], kind, me, c).wait_send()
            remote(INNER, 2, got.at[kind, me], kind, me, c).wait_send()
            for slot in range(3):
                remote(OUTER, slot, got.at[kind, me], kind, me, c).wait_send()


def body(image_emb, text_emb, positives, pair_mask, log_scale, bias):
    reach = (pair_mask.shape[1] - 1) // 2
    block_count = lax.axis_size("blk")
    row_count, width = image_emb.shape
    if block_count != 2 * (reach + 1) or reach != 3 or row_count % (3 * 128) != 0:
        return plain_body(image_emb, text_emb, positives, pair_mask, log_scale, bias)
    parts, tiles = 6, 3
    groups = lax.axis_size("grp")
    smem = pl.BlockSpec(memory_space=pltpu.SMEM)
    anywhere = pl.BlockSpec(memory_space=pl.ANY)
    return pl.pallas_call(
        functools.partial(grid_kernel, reach, parts, tiles),
        out_shape=(
            jax.ShapeDtypeStruct(image_emb.shape, image_emb.dtype),
            jax.ShapeDtypeStruct(text_emb.shape, text_emb.dtype),
            jax.ShapeDtypeStruct((1,), jnp.float32),
        ),
        in_specs=[smem] * 3 + [anywhere] * 3,
        out_specs=(anywhere, anywhere, smem),
        scratch_shapes=[
            pltpu.VMEM((2, row_count, width), jnp.bfloat16),
            pltpu.VMEM((1, row_count), jnp.int32),
            pltpu.VMEM((2, row_count, width), jnp.bfloat16),
            pltpu.VMEM((2, block_count, row_count, width), jnp.bfloat16),
            pltpu.VMEM((2, row_count, width), jnp.bfloat16),
            pltpu.VMEM((row_count, width), jnp.bfloat16),
            pltpu.VMEM((2, row_count, width), jnp.float32),
            pltpu.VMEM((1, row_count), jnp.float32),
            pltpu.VMEM((block_count, 8, 128), jnp.float32),
            pltpu.VMEM((groups, 8, 128), jnp.float32),
            pltpu.SemaphoreType.DMA((3,)),
            pltpu.SemaphoreType.DMA((2, tiles)),
            pltpu.SemaphoreType.DMA((3, 3, 2, parts)),
            pltpu.SemaphoreType.DMA((2, block_count, parts)),
            pltpu.SemaphoreType.DMA((block_count,)),
            pltpu.SemaphoreType.DMA((block_count,)),
            pltpu.SemaphoreType.DMA((groups,)),
            pltpu.SemaphoreType.DMA((groups,)),
        ],
        compiler_params=pltpu.CompilerParams(
            collective_id=0, has_side_effects=True, vmem_limit_bytes=67043328
        ),
    )(pair_mask, log_scale, bias, image_emb, text_emb, positives)


def solution(mesh):
    return jax.shard_map(
        body,
        mesh=mesh,
        in_specs=(
            P(("blk", "grp"), None),
            P(("blk", "grp"), None),
            P(("blk", "grp"), None),
            P(),
            P(),
            P(),
        ),
        out_specs=(P(("blk", "grp"), None), P(("blk", "grp"), None), P()),
        check_vma=False,
    )
```
